8 devices in a mesh: dp: 1 (over z), ctx: 8 (over y, x, core).
Axes of the slice: x: 2, y: 2, z: 1, core: 2. Of those that a mesh axis runs over, the one named last changes fastest.
Arguments:
- x_chunk: bfloat16 [2048, 2560], P(('dp', 'ctx'))
- cache_len: int32 [1], P('dp')
- k_cache: bfloat16 [2, 16384, 20, 128], P(None, ('dp', 'ctx'))
- v_cache: bfloat16 [2, 16384, 20, 128], P(None, ('dp', 'ctx'))
- k_local: bfloat16 [2, 256, 20, 128], P(None, 'dp')
- v_local: bfloat16 [2, 256, 20, 128], P(None, 'dp')
- g_attn: bfloat16 [4, 2560], replicated
- g_mlp: bfloat16 [4, 2560], replicated
- w_q: bfloat16 [4, 2560, 2560], replicated
- w_k: bfloat16 [4, 2560, 2560], replicated
- w_v: bfloat16 [4, 2560, 2560], replicated
- w_o: bfloat16 [4, 2560, 2560], replicated
- w_gate: bfloat16 [4, 2560, 10240], replicated
- w_up: bfloat16 [4, 2560, 10240], replicated
- w_down: bfloat16 [4, 10240, 2560], replicated
Outputs:
- output: bfloat16 [2048, 2560], P(('dp', 'ctx'))
All inputs are finite; a program needn't handle non-finite values.
Results may differ from the reference program's by a relative error of at most 0.02.
Values are sent between devices in bfloat16 or wider.
A program may use at most 3.5 GiB of HBM per device.

```python
import math
import jax
import jax.numpy as jnp
from jax import lax

D_MODEL = 2560
NUM_HEADS = 20
KV_HEADS = 20
HEAD_DIM = 128
WINDOW = 256
FF_DIM = 10240
SEQ_NEW = 2048
CACHE_SIZE = 16384
QUERY_ROWS = 128
NUM_PAIRS = 2
NORM_EPS = 1e-6


def draw_normal(rng_key, arr_shape, factor):
    return jax.random.normal(rng_key, arr_shape, jnp.float32) * factor


def setup_inputs(seed: int = 0, part: int = 0) -> dict:
    part_keys = jax.random.split(jax.random.fold_in(jax.random.key(seed), part), 6)
    shared_keys = jax.random.split(jax.random.key(seed + 1), 9)
    n_layers = 2 * NUM_PAIRS
    q_width = NUM_HEADS * HEAD_DIM
    kv_width = KV_HEADS * HEAD_DIM
    gain_local = math.log(max(WINDOW / 8.0, 2.0)) ** 0.25
    gain_global = math.log(max((CACHE_SIZE + SEQ_NEW) / 16.0, 2.0)) ** 0.25
    gain_base = jnp.tile(jnp.array([gain_local, gain_global], jnp.float32), NUM_PAIRS)
    cache_shape = (NUM_PAIRS, CACHE_SIZE, KV_HEADS, HEAD_DIM)
    local_shape = (NUM_PAIRS, WINDOW, KV_HEADS, HEAD_DIM)
    x_chunk = draw_normal(part_keys[0], (SEQ_NEW, D_MODEL), 1.0).astype(jnp.bfloat16)
    cache_len = jax.random.randint(part_keys[1], (1,), CACHE_SIZE // 2, CACHE_SIZE + 1, jnp.int32)
    k_cache = draw_normal(part_keys[2], cache_shape, gain_global).astype(jnp.bfloat16)
    v_cache = draw_normal(part_keys[3], cache_shape, gain_global).astype(jnp.bfloat16)
    k_local = draw_normal(part_keys[4], local_shape, gain_local).astype(jnp.bfloat16)
    v_local = draw_normal(part_keys[5], local_shape, gain_local).astype(jnp.bfloat16)
    g_attn = (gain_base[:, None] * (1.0 + draw_normal(shared_keys[0], (n_layers, D_MODEL), 0.2))).astype(jnp.bfloat16)
    g_mlp = (1.0 + draw_normal(shared_keys[1], (n_layers, D_MODEL), 0.2)).astype(jnp.bfloat16)
    w_q = draw_normal(shared_keys[2], (n_layers, D_MODEL, q_width), D_MODEL ** -0.5).astype(jnp.bfloat16)
    w_k = draw_normal(shared_keys[3], (n_layers, D_MODEL, kv_width), D_MODEL ** -0.5).astype(jnp.bfloat16)
    w_v = draw_normal(shared_keys[4], (n_layers, D_MODEL, kv_width), D_MODEL ** -0.5).astype(jnp.bfloat16)
    w_o = draw_normal(shared_keys[5], (n_layers, q_width, D_MODEL), q_width ** -0.5).astype(jnp.bfloat16)
    w_gate = draw_normal(shared_keys[6], (n_layers, D_MODEL, FF_DIM), D_MODEL ** -0.5).astype(jnp.bfloat16)
    w_up = draw_normal(shared_keys[7], (n_layers, D_MODEL, FF_DIM), D_MODEL ** -0.5).astype(jnp.bfloat16)
    w_down = draw_normal(shared_keys[8], (n_layers, FF_DIM, D_MODEL), FF_DIM ** -0.5).astype(jnp.bfloat16)
    return {'x_chunk': x_chunk, 'cache_len': cache_len, 'k_cache': k_cache, 'v_cache': v_cache,
            'k_local': k_local, 'v_local': v_local, 'g_attn': g_attn, 'g_mlp': g_mlp,
            'w_q': w_q, 'w_k': w_k, 'w_v': w_v, 'w_o': w_o,
            'w_gate': w_gate, 'w_up': w_up, 'w_down': w_down}


def rms_norm(rows_in, gain_vec):
    rows_f32 = rows_in.astype(jnp.float32)
    inv_rms = lax.rsqrt(jnp.mean(rows_f32 * rows_f32, axis=-1, keepdims=True) + NORM_EPS)
    return (rows_f32 * inv_rms * gain_vec.astype(jnp.float32)).astype(jnp.bfloat16)


def project(rows_in, weight):
    return jnp.dot(rows_in, weight, preferred_element_type=jnp.float32).astype(jnp.bfloat16)


def qkv_heads(normed, w_query, w_key, w_value):
    groups = NUM_HEADS // KV_HEADS
    queries = project(normed, w_query).reshape(SEQ_NEW, KV_HEADS, groups, HEAD_DIM)
    new_k = project(normed, w_key).reshape(SEQ_NEW, KV_HEADS, HEAD_DIM)
    new_v = project(normed, w_value).reshape(SEQ_NEW, KV_HEADS, HEAD_DIM)
    return queries, new_k, new_v


def attend(score_list, value_list):
    row_max = score_list[0].max(axis=-1)
    for part_scores in score_list[1:]:
        row_max = jnp.maximum(row_max, part_scores.max(axis=-1))
    row_sum = 0.0
    weighted = 0.0
    for part_scores, part_values in zip(score_list, value_list):
        part_probs = jnp.exp(part_scores - row_max[..., None])
        row_sum = row_sum + part_probs.sum(axis=-1)
        weighted = weighted + jnp.einsum('hgqk,khd->qhgd', part_probs.astype(jnp.bfloat16).astype(jnp.float32), part_values.astype(jnp.float32))
    return (weighted / jnp.transpose(row_sum, (2, 0, 1))[..., None]).astype(jnp.bfloat16)


def local_attention(queries, ext_k, ext_v):
    score_scale = HEAD_DIM ** -0.5
    rel_pos = jnp.arange(WINDOW + QUERY_ROWS)[None, :] - jnp.arange(QUERY_ROWS)[:, None]
    band_mask = (rel_pos > 0) & (rel_pos <= WINDOW)

    def one_block(block_idx):
        row_start = block_idx * QUERY_ROWS
        q_rows = lax.dynamic_slice_in_dim(queries, row_start, QUERY_ROWS, axis=0).astype(jnp.float32)
        k_rows = lax.dynamic_slice_in_dim(ext_k, row_start, WINDOW + QUERY_ROWS, axis=0)
        v_rows = lax.dynamic_slice_in_dim(ext_v, row_start, WINDOW + QUERY_ROWS, axis=0)
        scores = jnp.einsum('qhgd,khd->hgqk', q_rows, k_rows.astype(jnp.float32)) * score_scale
        scores = jnp.where(band_mask, scores, -jnp.inf)
        return attend([scores], [v_rows])

    blocks = lax.map(one_block, jnp.arange(SEQ_NEW // QUERY_ROWS))
    return blocks.reshape(SEQ_NEW, NUM_HEADS * HEAD_DIM)


def global_attention(queries, cache_k, cache_v, new_k, new_v, valid_len):
    score_scale = HEAD_DIM ** -0.5
    cache_mask = jnp.arange(CACHE_SIZE) < valid_len
    new_pos = jnp.arange(SEQ_NEW)
    cache_f32 = cache_k.astype(jnp.float32)
    new_f32 = new_k.astype(jnp.float32)

    def one_block(block_idx):
        row_start = block_idx * QUERY_ROWS
        q_rows = lax.dynamic_slice_in_dim(queries, row_start, QUERY_ROWS, axis=0).astype(jnp.float32)
        q_pos = row_start + jnp.arange(QUERY_ROWS)
        cache_scores = jnp.einsum('qhgd,khd->hgqk', q_rows, cache_f32) * score_scale
        cache_scores = jnp.where(cache_mask, cache_scores, -jnp.inf)
        new_scores = jnp.einsum('qhgd,khd->hgqk', q_rows, new_f32) * score_scale
        new_scores = jnp.where(new_pos[None, :] <= q_pos[:, None], new_scores, -jnp.inf)
        return attend([cache_scores, new_scores], [cache_v, new_v])

    blocks = lax.map(one_block, jnp.arange(SEQ_NEW // QUERY_ROWS))
    return blocks.reshape(SEQ_NEW, NUM_HEADS * HEAD_DIM)


def add_residual(hidden, attn_out, w_out):
    return (hidden.astype(jnp.float32) + jnp.dot(attn_out, w_out, preferred_element_type=jnp.float32)).astype(jnp.bfloat16)


def mlp_block(hidden, gain_vec, w_gate, w_up, w_down):
    normed = rms_norm(hidden, gain_vec)
    gate_pre = jnp.dot(normed, w_gate, preferred_element_type=jnp.float32)
    up_pre = jnp.dot(normed, w_up, preferred_element_type=jnp.float32)
    act_bf16 = (jax.nn.gelu(gate_pre, approximate=True) * up_pre).astype(jnp.bfloat16)
    return (hidden.astype(jnp.float32) + jnp.dot(act_bf16, w_down, preferred_element_type=jnp.float32)).astype(jnp.bfloat16)


def reference(x_chunk, cache_len, k_cache, v_cache, k_local, v_local, g_attn, g_mlp, w_q, w_k, w_v, w_o, w_gate, w_up, w_down):
    hidden = x_chunk
    for pair_idx in range(NUM_PAIRS):
        layer_idx = 2 * pair_idx
        queries, new_k, new_v = qkv_heads(rms_norm(hidden, g_attn[layer_idx]), w_q[layer_idx], w_k[layer_idx], w_v[layer_idx])
        ext_k = jnp.concatenate([k_local[pair_idx], new_k], axis=0)
        ext_v = jnp.concatenate([v_local[pair_idx], new_v], axis=0)
        attn_out = local_attention(queries, ext_k, ext_v)
        hidden = add_residual(hidden, attn_out, w_o[layer_idx])
        hidden = mlp_block(hidden, g_mlp[layer_idx], w_gate[layer_idx], w_up[layer_idx], w_down[layer_idx])
        layer_idx = 2 * pair_idx + 1
        queries, new_k, new_v = qkv_heads(rms_norm(hidden, g_attn[layer_idx]), w_q[layer_idx], w_k[layer_idx], w_v[layer_idx])
        attn_out = global_attention(queries, k_cache[pair_idx], v_cache[pair_idx], new_k, new_v, cache_len[0])
        hidden = add_residual(hidden, attn_out, w_o[layer_idx])
        hidden = mlp_block(hidden, g_mlp[layer_idx], w_gate[layer_idx], w_up[layer_idx], w_down[layer_idx])
    return hidden
```

```python
import functools
import jax
import jax.numpy as jnp
from jax import lax
from jax.experimental import pallas as pl
from jax.experimental.pallas import tpu as pltpu
from jax.sharding import PartitionSpec as P

EPS = 1e-6
CH = 512
NS = 3
KT = 1024
HD = 128
LOG2E = 1.4426950408889634
SCALE2 = LOG2E * HD ** -0.5
NEG = -jnp.inf
BF = jnp.bfloat16
F32 = jnp.float32
VLIM = 60 * 2 ** 20

VM = pl.BlockSpec(memory_space=pltpu.VMEM)
HB = pl.BlockSpec(memory_space=pl.ANY)
SM = pl.BlockSpec(memory_space=pltpu.SMEM)


def norm_rows(xf, gain):
    inv = lax.rsqrt(jnp.mean(xf * xf, axis=-1, keepdims=True) + EPS)
    return (xf * inv * gain).astype(BF)


def col(c, w):
    return pl.ds(pl.multiple_of(c * w, w), w)


def put_heads(dst, idx, src, n_chip, width):
    for g in range(n_chip):
        dst[(g,) + idx] = src[:, g * width:(g + 1) * width]


def layer_kernel(layer, nxt, split, rows, d, ff, n_chip):
    has_tail = layer is not None
    na = d // CH if has_tail else 0
    nb = ff // CH if has_tail else 0
    nq = d // CH
    nc = 3 * nq if nxt is not None else 0
    total = na + nb + nc
    width = d // n_chip

    def body(*refs):
        refs = list(refs)
        if has_tail:
            o_ref = refs.pop(0)
        x_ref = refs.pop(0)
        if has_tail:
            gm_ref = refs.pop(0)
        if nc:
            ga_ref = refs.pop(0)
        if has_tail:
            wo, wg, wu, wd = [refs.pop(0) for _ in range(4)]
        if nc:
            wq, wk, wv = [refs.pop(0) for _ in range(3)]
        if has_tail:
            xo_ref = refs.pop(0)
        if nc:
            if split:
                q_ref, kv_ref = refs.pop(0), refs.pop(0)
            else:
                q_ref, k_ref, v_ref = refs.pop(0), refs.pop(0), refs.pop(0)
        ba, bb, bd, h_s, acc, y_s, sa, sb, sd = refs

        def cp(w, l, c, buf, sem, slot, by_rows=False):
            src = w.at[l, pl.ds(pl.multiple_of(c * CH, CH), CH), :] if by_rows else w.at[l, :, col(c, CH)]
            return pltpu.make_async_copy(src, buf.at[slot], sem.at[slot])

        def start(t):
            slot = lax.rem(t, NS)
            if has_tail:
                @pl.when(t < na)
                def _():
                    cp(wo, layer, t, bd, sd, slot, True).start()

                @pl.when((t >= na) & (t < na + nb))
                def _():
                    c = t - na
                    cp(wg, layer, c, ba, sa, slot).start()
                    cp(wu, layer, c, bb, sb, slot).start()
                    cp(wd, layer, c, bd, sd, slot, True).start()
            if nc:
                for i, w in enumerate((wq, wk, wv)):
                    lo = na + nb + i * nq

                    @pl.when((t >= lo) & (t < lo + nq))
                    def _():
                        cp(w, nxt, t - lo, ba, sa, slot).start()

        for t in range(NS - 1):
            start(jnp.int32(t))
        if has_tail:
            for g in range(n_chip):
                y_s[:, g * width:(g + 1) * width] = o_ref[g]
            acc[...] = x_ref[...].astype(F32)

            def pa(t, _):
                start(t + NS - 1)
                slot = lax.rem(t, NS)
                cp(wo, layer, 0, bd, sd, slot, True).wait()
                acc[...] += jnp.dot(y_s[:, col(t, CH)], bd[slot], preferred_element_type=F32)
                return 0
            lax.fori_loop(0, na, pa, 0)
            xm = acc[...].astype(BF).astype(F32)
            h_s[...] = norm_rows(xm, gm_ref[layer:layer + 1, :].astype(F32))
            acc[...] = xm

            def pb(t, _):
                @pl.when(t + NS - 1 < total)
                def _():
                    start(t + NS - 1)
                slot = lax.rem(t, NS)
                cp(wg, layer, 0, ba, sa, slot).wait()
                gate = jnp.dot(h_s[...], ba[slot], preferred_element_type=F32)
                cp(wu, layer, 0, bb, sb, slot).wait()
                up = jnp.dot(h_s[...], bb[slot], preferred_element_type=F32)
                act = (jax.nn.gelu(gate, approximate=True) * up).astype(BF)
                cp(wd, layer, 0, bd, sd, slot, True).wait()
                acc[...] += jnp.dot(act, bd[slot], preferred_element_type=F32)
                return 0
            lax.fori_loop(na, na + nb, pb, 0)
            xb = acc[...].astype(BF)
            xo_ref[...] = xb
        else:
            xb = x_ref[...]
        if nc:
            h_s[...] = norm_rows(xb.astype(F32), ga_ref[nxt:nxt + 1, :].astype(F32))
            for i, w in enumerate((wq, wk, wv)):
                lo = na + nb + i * nq

                def pc(t, _):
                    @pl.when(t + NS - 1 < total)
                    def _():
                        start(t + NS - 1)
                    slot = lax.rem(t, NS)
                    cp(w, nxt, 0, ba, sa, slot).wait()
                    y = jnp.dot(h_s[...], ba[slot], preferred_element_type=F32).astype(BF)
                    if split:
                        y_s[:, col(t - lo, CH)] = y
                    else:
                        (q_ref, k_ref, v_ref)[i][:, col(t - lo, CH)] = y
                    return 0
                lax.fori_loop(lo, lo + nq, pc, 0)
                if split:
                    if i == 0:
                        put_heads(q_ref, (), y_s, n_chip, width)
                    else:
                        put_heads(kv_ref, (i - 1,), y_s, n_chip, width)

    n_in_v = (3 if has_tail else 1) + (1 if nc else 0)
    n_in_h = (4 if has_tail else 0) + (3 if nc else 0)
    outs = []
    if has_tail:
        outs.append(jax.ShapeDtypeStruct((rows, d), BF))
    if nc:
        if split:
            outs += [jax.ShapeDtypeStruct((n_chip, rows, width), BF), jax.ShapeDtypeStruct((n_chip, 2, rows, width), BF)]
        else:
            outs += [jax.ShapeDtypeStruct((rows, d), BF)] * 3
    flops = 2 * rows * d * ((d + 3 * ff if has_tail else 0) + (3 * d if nc else 0))
    return pl.pallas_call(
        body, out_shape=outs, in_specs=[VM] * n_in_v + [HB] * n_in_h, out_specs=[VM] * len(outs),
        scratch_shapes=[
            pltpu.VMEM((NS, d, CH), BF), pltpu.VMEM((NS, d, CH), BF), pltpu.VMEM((NS, CH, d), BF),
            pltpu.VMEM((rows, d), BF), pltpu.VMEM((rows, d), F32), pltpu.VMEM((rows, d), BF),
            pltpu.SemaphoreType.DMA((NS,)), pltpu.SemaphoreType.DMA((NS,)), pltpu.SemaphoreType.DMA((NS,))],
        compiler_params=pltpu.CompilerParams(vmem_limit_bytes=VLIM),
        cost_estimate=pl.CostEstimate(flops=flops, bytes_accessed=flops // rows, transcendentals=0),
        name=f"layer_{layer}_{nxt}")


def local_attention(pair, rows, d, n_chip):
    hg = d // HD // n_chip
    width = d // n_chip

    def body(dev_ref, q_ref, k_ref, v_ref, kh_ref, vh_ref, kl_ref, vl_ref, o_ref):
        first = dev_ref[0] == 0
        key_id = lax.broadcasted_iota(jnp.int32, (2 * rows, rows), 0)
        row_id = lax.broadcasted_iota(jnp.int32, (2 * rows, rows), 1)
        band = (key_id > row_id) & (key_id <= row_id + rows)

        def chip(g, _):
            for j in range(hg):
                c = pl.ds(pl.multiple_of(g * width + j * HD, HD), HD)
                k = jnp.concatenate([jnp.where(first, kl_ref[0, g * hg + j], kh_ref[:, c]), k_ref[:, c]], axis=0)
                v = jnp.concatenate([jnp.where(first, vl_ref[0, g * hg + j], vh_ref[:, c]), v_ref[:, c]], axis=0)
                s = lax.dot_general(k, q_ref[:, c], (((1,), (1,)), ((), ())), preferred_element_type=F32)
                s = jnp.where(band, s, NEG)
                m = jnp.max(s, axis=0, keepdims=True)
                p = jnp.exp2(s * SCALE2 - m * SCALE2)
                l = jnp.sum(p, axis=0, keepdims=True)
                o = lax.dot_general(v, p.astype(BF), (((0,), (0,)), ((), ())), preferred_element_type=F32)
                o_ref[g, :, j * HD:(j + 1) * HD] = (o / l).T.astype(BF)
            return 0
        lax.fori_loop(0, n_chip, chip, 0)

    loc = pl.BlockSpec((1, d // HD, rows, HD), lambda i: (pair, 0, 0, 0))
    return pl.pallas_call(
        body, grid=(1,), out_shape=jax.ShapeDtypeStruct((n_chip, rows, width), BF),
        in_specs=[SM] + [VM] * 5 + [loc, loc], out_specs=pl.BlockSpec((n_chip, rows, width), lambda i: (0, 0, 0)),
        compiler_params=pltpu.CompilerParams(vmem_limit_bytes=VLIM),
        cost_estimate=pl.CostEstimate(flops=8 * rows * rows * d, bytes_accessed=16 * rows * d, transcendentals=0),
        name=f"local_{pair}")


def global_attention(pair, slot_rows, rows, hg, n_chip):
    cache = 2 * n_chip * slot_rows
    new = 2 * n_chip * rows
    nq = n_chip * rows

    def body(core_ref, len_ref, q_ref, ka, kp, va, vp, kv, kvp, o_ref, ks, vs, m_s, l_s, acc, s_a, s_b, sk, sv):
        h = pl.program_id(0)
        c = core_ref[0]
        n = len_ref[0]

        def copies(hh, slot):
            out = []
            for g in range(n_chip):
                for par, (kk, vv, nn) in enumerate(((ka, va, kv), (kp, vp, kvp))):
                    dev = 2 * g + (c if par == 0 else 1 - c)
                    r = pl.ds(pl.multiple_of(dev * slot_rows, slot_rows), slot_rows)
                    out.append(pltpu.make_async_copy(kk.at[g, hh], ks.at[slot, r, :], sk.at[slot]))
                    out.append(pltpu.make_async_copy(vv.at[g, hh], vs.at[slot, r, :], sv.at[slot]))
                    r = pl.ds(pl.multiple_of(cache + dev * rows, rows), rows)
                    out.append(pltpu.make_async_copy(nn.at[g, 0, :, col(hh, HD)], ks.at[slot, r, :], sk.at[slot]))
                    out.append(pltpu.make_async_copy(nn.at[g, 1, :, col(hh, HD)], vs.at[slot, r, :], sv.at[slot]))
            return out

        slot = lax.rem(h, 2)

        @pl.when(h == 0)
        def _():
            for x in copies(h, slot):
                x.start()

        @pl.when(h + 1 < hg)
        def _():
            for x in copies(h + 1, 1 - slot):
                x.start()
        for x in copies(h, slot):
            x.wait()
        m_s[...] = jnp.full(m_s.shape, NEG, F32)
        l_s[...] = jnp.zeros(l_s.shape, F32)
        acc[...] = jnp.zeros(acc.shape, F32)
        q = q_ref[...].reshape(nq, HD)

        def scores(start, lo=0):
            k = ks[slot, pl.ds(start, KT), :]
            return lax.dot_general(k, q[lo:], (((1,), (1,)), ((), ())), preferred_element_type=F32)

        def absorb(s, start, lo=0):
            v = vs[slot, pl.ds(start, KT), :]
            m0 = m_s[:, lo:]
            m1 = jnp.maximum(m0, jnp.max(s, axis=0, keepdims=True))
            a = jnp.exp2((m0 - m1) * SCALE2)
            p = jnp.exp2(s * SCALE2 - m1 * SCALE2)
            l_s[:, lo:] = l_s[:, lo:] * a + jnp.sum(p, axis=0, keepdims=True)
            m_s[:, lo:] = m1
            acc[:, lo:] = acc[:, lo:] * a + lax.dot_general(v, p.astype(BF), (((0,), (0,)), ((), ())), preferred_element_type=F32)

        def tile(i):
            return pl.multiple_of(i * KT, KT)

        n_full = n // KT
        n_pair = n_full // 2
        s_a[...] = scores(0)

        def two(i, _):
            s_b[...] = scores(tile(2 * i + 1))
            absorb(s_a[...], tile(2 * i))
            s_a[...] = scores(tile(2 * i + 2))
            absorb(s_b[...], tile(2 * i + 1))
            return 0
        lax.fori_loop(0, n_pair, two, 0)

        @pl.when(n_full > 2 * n_pair)
        def _():
            absorb(scores(tile(n_full - 1)), tile(n_full - 1))
        left = n - n_full * KT

        @pl.when(left > 0)
        def _():
            s = scores(tile(n_full))
            keep = lax.broadcasted_iota(jnp.int32, s.shape, 0) < left
            absorb(jnp.where(keep, s, NEG), tile(n_full))
        for t in range(new // KT):
            lo = (t * KT) // (2 * rows) * rows
            s = scores(cache + t * KT, lo)
            qi = lax.broadcasted_iota(jnp.int32, s.shape, 1) + lo
            pos = (2 * (qi // rows) + c) * rows + qi % rows
            keep = lax.broadcasted_iota(jnp.int32, s.shape, 0) + t * KT <= pos
            absorb(jnp.where(keep, s, NEG), cache + t * KT, lo)
        for g in range(n_chip):
            r = slice(g * rows, (g + 1) * rows)
            o_ref[g] = (acc[:, r] / l_s[:, r]).T.astype(BF)

    flops = 4 * nq * (cache + new) * HD * hg
    return pl.pallas_call(
        body, grid=(hg,), out_shape=jax.ShapeDtypeStruct((n_chip, rows, hg * HD), BF),
        in_specs=[SM, SM, pl.BlockSpec((n_chip, rows, HD), lambda h: (0, 0, h))] + [HB] * 6,
        out_specs=pl.BlockSpec((n_chip, rows, HD), lambda h: (0, 0, h)),
        scratch_shapes=[pltpu.VMEM((2, cache + new, HD), BF)] * 2
        + [pltpu.VMEM((1, nq), F32)] * 2 + [pltpu.VMEM((HD, nq), F32)]
        + [pltpu.VMEM((KT, nq), F32)] * 2 + [pltpu.SemaphoreType.DMA((2,))] * 2,
        compiler_params=pltpu.CompilerParams(vmem_limit_bytes=VLIM, dimension_semantics=("arbitrary",)),
        cost_estimate=pl.CostEstimate(flops=flops, bytes_accessed=4 * (cache + new) * HD * hg, transcendentals=0),
        name=f"global_{pair}")


def solution(mesh):
    n_dev = mesh.shape['ctx']
    n_chip = n_dev // 2
    groups = [[2 * g + c for g in range(n_chip)] for c in range(2)]
    shift = [(i, i + 1) for i in range(n_dev - 1)]
    partner = [(i, i ^ 1) for i in range(n_dev)]
    row_spec = P(('dp', 'ctx'), None)
    cache_spec = P(None, ('dp', 'ctx'), None, None)
    local_spec = P(None, 'dp', None, None)
    in_specs = (row_spec, P('dp'), cache_spec, cache_spec, local_spec, local_spec) + (P(),) * 9

    def swap(x):
        return lax.all_to_all(x, 'ctx', 0, 0, axis_index_groups=groups)

    def step(x, cache_len, k_cache, v_cache, k_local, v_local, g_attn, g_mlp, w_q, w_k, w_v, w_o, w_gate, w_up, w_down):
        dev = lax.axis_index('ctx').astype(jnp.int32)
        dev_a = dev.reshape(1)
        core_a = lax.rem(dev, jnp.int32(2)).reshape(1)
        rows, d = x.shape
        ff = w_gate.shape[2]
        pairs, slots, heads, _ = k_cache.shape
        hg = heads // n_chip
        kc = jnp.transpose(k_cache, (0, 2, 1, 3))
        vc = jnp.transpose(v_cache, (0, 2, 1, 3))
        kl = jnp.transpose(k_local, (0, 2, 1, 3))
        vl = jnp.transpose(v_local, (0, 2, 1, 3))
        cache = []
        for p in range(pairs):
            ka = swap(kc[p].reshape(n_chip, hg, slots, HD))
            va = swap(vc[p].reshape(n_chip, hg, slots, HD))
            cache.append((ka, lax.ppermute(ka, 'ctx', partner), va, lax.ppermute(va, 'ctx', partner)))

        q, k, v = layer_kernel(None, 0, False, rows, d, ff, n_chip)(x, g_attn, w_q, w_k, w_v)
        for p in range(pairs):
            l = 2 * p
            kh = lax.ppermute(k, 'ctx', shift)
            vh = lax.ppermute(v, 'ctx', shift)
            o = local_attention(p, rows, d, n_chip)(dev_a, q, k, v, kh, vh, kl, vl)
            x, q4, kv = layer_kernel(l, l + 1, True, rows, d, ff, n_chip)(
                o, x, g_mlp, g_attn, w_o, w_gate, w_up, w_down, w_q, w_k, w_v)
            kv = swap(kv)
            kvp = lax.ppermute(kv, 'ctx', partner)
            q4 = swap(q4)
            o = global_attention(p, slots, rows, hg, n_chip)(core_a, cache_len, q4, *[cache[p][i] for i in range(4)], kv, kvp)
            o = swap(o)
            if p + 1 < pairs:
                x, q, k, v = layer_kernel(l + 1, l + 2, False, rows, d, ff, n_chip)(
                    o, x, g_mlp, g_attn, w_o, w_gate, w_up, w_down, w_q, w_k, w_v)
            else:
                x, = layer_kernel(l + 1, None, False, rows, d, ff, n_chip)(o, x, g_mlp, w_o, w_gate, w_up, w_down)
        return x

    return jax.shard_map(step, mesh=mesh, in_specs=in_specs, out_specs=row_spec, check_vma=False)
```

```python
import functools
import jax
import jax.numpy as jnp
from jax import lax
from jax.experimental import pallas as pl
from jax.experimental.pallas import tpu as pltpu
from jax.sharding import PartitionSpec as P

EPS = 1e-6
CH = 512
NS = 3
KT = 1024
HD = 128
LOG2E = 1.4426950408889634
SCALE2 = LOG2E * HD ** -0.5
NEG = -jnp.inf
BF = jnp.bfloat16
F32 = jnp.float32
VLIM = 60 * 2 ** 20

VM = pl.BlockSpec(memory_space=pltpu.VMEM)
HB = pl.BlockSpec(memory_space=pl.ANY)
SM = pl.BlockSpec(memory_space=pltpu.SMEM)


def norm_rows(xf, gain):
    inv = lax.rsqrt(jnp.mean(xf * xf, axis=-1, keepdims=True) + EPS)
    return (xf * inv * gain).astype(BF)


def col(c, w):
    return pl.ds(pl.multiple_of(c * w, w), w)


def layer_kernel(layer, nxt, rows, d, ff):
    has_tail = layer is not None
    na = d // CH if has_tail else 0
    nb = ff // CH if has_tail else 0
    nq = d // CH
    nc = 3 * nq if nxt is not None else 0
    total = na + nb + nc

    def body(*refs):
        refs = list(refs)
        if has_tail:
            o_ref = refs.pop(0)
        x_ref = refs.pop(0)
        if has_tail:
            gm_ref = refs.pop(0)
        if nc:
            ga_ref = refs.pop(0)
        if has_tail:
            wo, wg, wu, wd = [refs.pop(0) for _ in range(4)]
        if nc:
            wq, wk, wv = [refs.pop(0) for _ in range(3)]
        if has_tail:
            xo_ref = refs.pop(0)
        if nc:
            qkv_refs = [refs.pop(0) for _ in range(3)]
        ba, bb, bd, h_s, acc, sa, sb, sd = refs

        def cp(w, l, c, buf, sem, slot, by_rows=False):
            src = w.at[l, pl.ds(pl.multiple_of(c * CH, CH), CH), :] if by_rows else w.at[l, :, col(c, CH)]
            return pltpu.make_async_copy(src, buf.at[slot], sem.at[slot])

        def start(t):
            slot = lax.rem(t, NS)
            if has_tail:
                @pl.when(t < na)
                def _():
                    cp(wo, layer, t, bd, sd, slot, True).start()

                @pl.when((t >= na) & (t < na + nb))
                def _():
                    c = t - na
                    cp(wg, layer, c, ba, sa, slot).start()
                    cp(wu, layer, c, bb, sb, slot).start()
                    cp(wd, layer, c, bd, sd, slot, True).start()
            if nc:
                for i, w in enumerate((wq, wk, wv)):
                    lo = na + nb + i * nq

                    @pl.when((t >= lo) & (t < lo + nq))
                    def _():
                        cp(w, nxt, t - lo, ba, sa, slot).start()

        for t in range(NS - 1):
            start(jnp.int32(t))
        if has_tail:
            acc[...] = x_ref[...].astype(F32)

            def pa(t, _):
                start(t + NS - 1)
                slot = lax.rem(t, NS)
                cp(wo, layer, 0, bd, sd, slot, True).wait()
                acc[...] += jnp.dot(o_ref[:, col(t, CH)], bd[slot], preferred_element_type=F32)
                return 0
            lax.fori_loop(0, na, pa, 0)
            xm = acc[...].astype(BF).astype(F32)
            h_s[...] = norm_rows(xm, gm_ref[layer:layer + 1, :].astype(F32))
            acc[...] = xm

            def pb(t, _):
                @pl.when(t + NS - 1 < total)
                def _():
                    start(t + NS - 1)
                slot = lax.rem(t, NS)
                cp(wg, layer, 0, ba, sa, slot).wait()
                gate = jnp.dot(h_s[...], ba[slot], preferred_element_type=F32)
                cp(wu, layer, 0, bb, sb, slot).wait()
                up = jnp.dot(h_s[...], bb[slot], preferred_element_type=F32)
                act = (jax.nn.gelu(gate, approximate=True) * up).astype(BF)
                cp(wd, layer, 0, bd, sd, slot, True).wait()
                acc[...] += jnp.dot(act, bd[slot], preferred_element_type=F32)
                return 0
            lax.fori_loop(na, na + nb, pb, 0)
            xb = acc[...].astype(BF)
            xo_ref[...] = xb
        else:
            xb = x_ref[...]
        if nc:
            h_s[...] = norm_rows(xb.astype(F32), ga_ref[nxt:nxt + 1, :].astype(F32))
            for i, w in enumerate((wq, wk, wv)):
                lo = na + nb + i * nq

                def pc(t, _):
                    @pl.when(t + NS - 1 < total)
                    def _():
                        start(t + NS - 1)
                    slot = lax.rem(t, NS)
                    cp(w, nxt, 0, ba, sa, slot).wait()
                    qkv_refs[i][:, col(t - lo, CH)] = jnp.dot(h_s[...], ba[slot], preferred_element_type=F32).astype(BF)
                    return 0
                lax.fori_loop(lo, lo + nq, pc, 0)

    n_in_v = (3 if has_tail else 1) + (1 if nc else 0)
    n_in_h = (4 if has_tail else 0) + (3 if nc else 0)
    outs = []
    if has_tail:
        outs.append(jax.ShapeDtypeStruct((rows, d), BF))
    if nc:
        outs += [jax.ShapeDtypeStruct((rows, d), BF)] * 3
    flops = 2 * rows * d * ((d + 3 * ff if has_tail else 0) + (3 * d if nc else 0))
    return pl.pallas_call(
        body, out_shape=outs, in_specs=[VM] * n_in_v + [HB] * n_in_h, out_specs=[VM] * len(outs),
        scratch_shapes=[
            pltpu.VMEM((NS, d, CH), BF), pltpu.VMEM((NS, d, CH), BF), pltpu.VMEM((NS, CH, d), BF),
            pltpu.VMEM((rows, d), BF), pltpu.VMEM((rows, d), F32),
            pltpu.SemaphoreType.DMA((NS,)), pltpu.SemaphoreType.DMA((NS,)), pltpu.SemaphoreType.DMA((NS,))],
        compiler_params=pltpu.CompilerParams(vmem_limit_bytes=VLIM),
        cost_estimate=pl.CostEstimate(flops=flops, bytes_accessed=flops // rows, transcendentals=0),
        name=f"layer_{layer}_{nxt}")


def local_attention(pair, rows, d, n_chip):
    hg = d // HD // n_chip
    width = d // n_chip

    def body(dev_ref, q_ref, k_ref, v_ref, kh_ref, vh_ref, kl_ref, vl_ref, o_ref):
        first = dev_ref[0] == 0
        key_id = lax.broadcasted_iota(jnp.int32, (2 * rows, rows), 0)
        row_id = lax.broadcasted_iota(jnp.int32, (2 * rows, rows), 1)
        band = (key_id > row_id) & (key_id <= row_id + rows)

        def chip(g, _):
            for j in range(hg):
                c = pl.ds(pl.multiple_of(g * width + j * HD, HD), HD)
                k = jnp.concatenate([jnp.where(first, kl_ref[0, g * hg + j], kh_ref[:, c]), k_ref[:, c]], axis=0)
                v = jnp.concatenate([jnp.where(first, vl_ref[0, g * hg + j], vh_ref[:, c]), v_ref[:, c]], axis=0)
                s = lax.dot_general(k, q_ref[:, c], (((1,), (1,)), ((), ())), preferred_element_type=F32)
                s = jnp.where(band, s, NEG)
                m = jnp.max(s, axis=0, keepdims=True)
                p = jnp.exp2(s * SCALE2 - m * SCALE2)
                l = jnp.sum(p, axis=0, keepdims=True)
                o = lax.dot_general(v, p.astype(BF), (((0,), (0,)), ((), ())), preferred_element_type=F32)
                o_ref[:, c] = (o / l).T.astype(BF)
            return 0
        lax.fori_loop(0, n_chip, chip, 0)

    loc = pl.BlockSpec((1, d // HD, rows, HD), lambda i: (pair, 0, 0, 0))
    return pl.pallas_call(
        body, grid=(1,), out_shape=jax.ShapeDtypeStruct((rows, d), BF),
        in_specs=[SM] + [VM] * 5 + [loc, loc], out_specs=pl.BlockSpec((rows, d), lambda i: (0, 0)),
        compiler_params=pltpu.CompilerParams(vmem_limit_bytes=VLIM),
        cost_estimate=pl.CostEstimate(flops=8 * rows * rows * d, bytes_accessed=16 * rows * d, transcendentals=0),
        name=f"local_{pair}")


def global_attention(pair, slot_rows, rows, d, n_chip):
    n_dev = 2 * n_chip
    nq = n_dev * rows
    qh = nq // 2
    heads = d // HD
    hh = heads // 2
    half = hh * HD
    cache = 2 * slot_rows
    keys = cache + 2 * rows
    st = HD + 8
    n_tile = cache // KT
    low = -3e38

    def body(len_ref, q_ref, kn_ref, vn_ref, kc, vc, o_ref, kx, vx,
             qb, knp, vnp, ks, vs, m_s, l_s, acc, s_a, s_b, stage, part,
             q_snd, q_rcv, x_snd, x_rcv, n_snd, n_rcv, p_snd, p_rcv, sk, sv):
        dev = lax.axis_index('ctx')
        core = lax.rem(dev, 2)
        g_me = lax.div(dev, 2)
        mate = dev + 1 - 2 * core

        def remote(src, dst, snd, rcv, to):
            return pltpu.make_async_remote_copy(
                src_ref=src, dst_ref=dst, send_sem=snd, recv_sem=rcv,
                device_id={'ctx': to}, device_id_type=pl.DeviceIdType.MESH)

        def head_cols(b, i):
            return pl.ds(pl.multiple_of((b * hh + i) * HD, HD), HD)

        def dev_rows(t):
            return pl.ds(pl.multiple_of(t * rows, rows), rows)

        def q_copy(i, k):
            to = lax.rem(dev + k, n_dev)
            return remote(q_ref.at[:, head_cols(lax.rem(to, 2), i)], qb.at[i, dev_rows(dev), :],
                          q_snd.at[i, k - 1], q_rcv.at[i, dev], to)

        def q_wait(i, k):
            src = lax.rem(dev + k, n_dev)
            remote(q_ref.at[:, head_cols(0, i)], qb.at[i, dev_rows(src), :],
                   q_snd.at[i, k - 1], q_rcv.at[i, src], src).wait_recv()

        def x_copy(i, w):
            src, dst = ((kc, kx), (vc, vx))[w]
            return remote(src.at[pair, (1 - core) * hh + i], dst.at[i], x_snd.at[w, i], x_rcv.at[w, i], mate)

        def n_copy(w):
            src, dst = ((kn_ref, knp), (vn_ref, vnp))[w]
            return remote(src.at[:, pl.ds(pl.multiple_of((1 - core) * half, half), half)], dst,
                          n_snd.at[w], n_rcv.at[w], mate)

        def p_copy(i, k):
            to = lax.rem(dev + k, n_dev)
            return remote(stage.at[i, to], part.at[core * hh + i, g_me],
                          p_snd.at[i, k - 1], p_rcv.at[core * hh + i, g_me], to)

        def own(i, slot, w):
            src, dst, sem = ((kc, ks, sk), (vc, vs, sv))[w]
            return pltpu.make_async_copy(src.at[pair, core * hh + i], dst.at[slot, 0:slot_rows, :], sem.at[slot, 0])

        def mated(i, slot, w):
            src, dst, sem = ((kx, ks, sk), (vx, vs, sv))[w]
            return pltpu.make_async_copy(src.at[i], dst.at[slot, slot_rows:cache, :], sem.at[slot, 1])

        bar = pltpu.get_barrier_semaphore()
        for k in range(1, n_dev):
            pl.semaphore_signal(bar, inc=1, device_id={'ctx': lax.rem(dev + k, n_dev)}, device_id_type=pl.DeviceIdType.MESH)
        pl.semaphore_wait(bar, n_dev - 1)

        for w in range(2):
            own(0, 0, w).start()
            x_copy(0, w).start()
            n_copy(w).start()

        def send_q(i, _):
            for k in range(1, n_dev):
                q_copy(i, k).start()
            return 0
        lax.fori_loop(0, hh, send_q, 0)

        def send_x(i, _):
            for w in range(2):
                x_copy(i, w).start()
            return 0
        lax.fori_loop(1, hh, send_x, 0)
        for w in range(2):
            x_copy(0, w).wait_recv()
            mated(0, 0, w).start()
            n_copy(w).wait_recv()

        n = len_ref[0]

        def one_head(i, _):
            slot = lax.rem(i, 2)

            @pl.when(i + 1 < hh)
            def _():
                for w in range(2):
                    own(i + 1, 1 - slot, w).start()
                    x_copy(i + 1, w).wait_recv()
                    mated(i + 1, 1 - slot, w).start()
            mine = head_cols(core, i)
            there = head_cols(0, i)
            ks[slot, cache:cache + rows, :] = kn_ref[:, mine]
            ks[slot, cache + rows:keys, :] = knp[:, there]
            vs[slot, cache:cache + rows, :] = vn_ref[:, mine]
            vs[slot, cache + rows:keys, :] = vnp[:, there]
            qb[i, dev_rows(dev), :] = q_ref[:, mine]
            m_s[...] = jnp.full(m_s.shape, low, F32)
            l_s[...] = jnp.zeros(l_s.shape, F32)
            acc[...] = jnp.zeros(acc.shape, F32)
            for k in range(1, n_dev):
                q_wait(i, k)
            for w in range(2):
                own(i, slot, w).wait()
                mated(i, slot, w).wait()

            def scores(start, size, hf):
                k = ks[slot, pl.ds(start, size), :]
                q = qb[i, hf * qh:(hf + 1) * qh, :]
                return lax.dot_general(k, q, (((1,), (1,)), ((), ())), preferred_element_type=F32)

            def absorb(s, start, size, hf):
                v = vs[slot, pl.ds(start, size), :]
                c = slice(hf * qh, (hf + 1) * qh)
                m0 = m_s[:, c]
                m1 = jnp.maximum(m0, jnp.max(s, axis=0, keepdims=True))
                a = jnp.exp2((m0 - m1) * SCALE2)
                p = jnp.exp2(s * SCALE2 - m1 * SCALE2)
                l_s[:, c] = l_s[:, c] * a + jnp.sum(p, axis=0, keepdims=True)
                m_s[:, c] = m1
                acc[:, c] = acc[:, c] * a + lax.dot_general(v, p.astype(BF), (((0,), (0,)), ((), ())), preferred_element_type=F32)

            def tile(t):
                return pl.multiple_of(t * KT, KT)

            def valid(s, t):
                per = slot_rows // KT
                owner = jnp.where(t < per, dev, mate)
                left = n - owner * slot_rows - lax.rem(t, per) * KT
                return jnp.where(lax.broadcasted_iota(jnp.int32, s.shape, 0) < left, s, NEG)

            s_a[...] = scores(0, KT, 0)

            def tiles(t, _):
                s_b[...] = scores(tile(t), KT, 1)
                absorb(valid(s_a[...], t), tile(t), KT, 0)
                s_a[...] = scores(tile(t + 1), KT, 0)
                absorb(valid(s_b[...], t), tile(t), KT, 1)
                return 0
            lax.fori_loop(0, n_tile - 1, tiles, 0)
            last = n_tile - 1
            s_b[...] = scores(last * KT, KT, 1)
            absorb(valid(s_a[...], last), last * KT, KT, 0)
            absorb(valid(s_b[...], last), last * KT, KT, 1)
            for hf in range(2):
                s = scores(cache, 2 * rows, hf)
                r = lax.broadcasted_iota(jnp.int32, s.shape, 0)
                qi = lax.broadcasted_iota(jnp.int32, s.shape, 1) + hf * qh
                pos = jnp.where(r < rows, r + dev * rows, r - rows + mate * rows)
                absorb(jnp.where(pos <= qi, s, NEG), cache, 2 * rows, hf)
            for t in range(n_dev):
                c = slice(t * rows, (t + 1) * rows)
                stage[i, t, 0:HD, :] = acc[:, c]
                stage[i, t, HD:HD + 1, :] = m_s[:, c]
                stage[i, t, HD + 1:HD + 2, :] = l_s[:, c]
            part[core * hh + i, g_me] = stage[i, dev]
            for k in range(1, n_dev):
                p_copy(i, k).start()
            return 0
        lax.fori_loop(0, hh, one_head, 0)

        def finish(i, _):
            for b in range(2):
                h = b * hh + i
                for g in range(n_chip):
                    src = 2 * g + b

                    @pl.when(src != dev)
                    def _():
                        remote(stage.at[i, 0], part.at[h, g], p_snd.at[i, 0], p_rcv.at[h, g], mate).wait_recv()
                m = [part[h, g, HD:HD + 1, :] for g in range(n_chip)]
                top = functools.reduce(jnp.maximum, m)
                num = 0.0
                den = 0.0
                for g in range(n_chip):
                    a = jnp.exp2((m[g] - top) * SCALE2)
                    num = num + part[h, g, 0:HD, :] * a
                    den = den + part[h, g, HD + 1:HD + 2, :] * a
                o_ref[:, head_cols(b, i)] = (num / den).T.astype(BF)
            return 0
        lax.fori_loop(0, hh, finish, 0)

        def drain(i, _):
            for k in range(1, n_dev):
                q_copy(i, k).wait_send()
                p_copy(i, k).wait_send()
            for w in range(2):
                x_copy(i, w).wait_send()
            return 0
        lax.fori_loop(0, hh, drain, 0)
        for w in range(2):
            n_copy(w).wait_send()

    flops = 4 * nq * keys * half
    dma = pltpu.SemaphoreType.DMA
    xs = jax.ShapeDtypeStruct((hh, slot_rows, HD), BF)
    return pl.pallas_call(
        body, out_shape=[jax.ShapeDtypeStruct((rows, d), BF), xs, xs],
        in_specs=[SM, VM, VM, VM, HB, HB], out_specs=[VM, HB, HB],
        scratch_shapes=[
            pltpu.VMEM((hh, nq, HD), BF), pltpu.VMEM((rows, half), BF), pltpu.VMEM((rows, half), BF),
            pltpu.VMEM((2, keys, HD), BF), pltpu.VMEM((2, keys, HD), BF),
            pltpu.VMEM((1, nq), F32), pltpu.VMEM((1, nq), F32), pltpu.VMEM((HD, nq), F32),
            pltpu.VMEM((KT, qh), F32), pltpu.VMEM((KT, qh), F32),
            pltpu.VMEM((hh, n_dev, st, rows), F32), pltpu.VMEM((heads, n_chip, st, rows), F32),
            dma((hh, n_dev - 1)), dma((hh, n_dev)), dma((2, hh)), dma((2, hh)), dma((2,)), dma((2,)),
            dma((hh, n_dev - 1)), dma((heads, n_chip)), dma((2, 2)), dma((2, 2))],
        compiler_params=pltpu.CompilerParams(vmem_limit_bytes=VLIM, collective_id=pair, has_side_effects=True),
        cost_estimate=pl.CostEstimate(flops=flops, bytes_accessed=4 * keys * half, transcendentals=0),
        name=f"global_{pair}")


def solution(mesh):
    n_dev = mesh.shape['ctx']
    n_chip = n_dev // 2
    shift = [(i, i + 1) for i in range(n_dev - 1)]
    row_spec = P(('dp', 'ctx'), None)
    cache_spec = P(None, ('dp', 'ctx'), None, None)
    local_spec = P(None, 'dp', None, None)
    in_specs = (row_spec, P('dp'), cache_spec, cache_spec, local_spec, local_spec) + (P(),) * 9

    def step(x, cache_len, k_cache, v_cache, k_local, v_local, g_attn, g_mlp, w_q, w_k, w_v, w_o, w_gate, w_up, w_down):
        dev_a = lax.axis_index('ctx').astype(jnp.int32).reshape(1)
        rows, d = x.shape
        ff = w_gate.shape[2]
        pairs, slots, _, _ = k_cache.shape
        kc = jnp.transpose(k_cache, (0, 2, 1, 3))
        vc = jnp.transpose(v_cache, (0, 2, 1, 3))
        kl = jnp.transpose(k_local, (0, 2, 1, 3))
        vl = jnp.transpose(v_local, (0, 2, 1, 3))
        q, k, v = layer_kernel(None, 0, rows, d, ff)(x, g_attn, w_q, w_k, w_v)
        for p in range(pairs):
            l = 2 * p
            kh = lax.ppermute(k, 'ctx', shift)
            vh = lax.ppermute(v, 'ctx', shift)
            o = local_attention(p, rows, d, n_chip)(dev_a, q, k, v, kh, vh, kl, vl)
            x, q, k, v = layer_kernel(l, l + 1, rows, d, ff)(
                o, x, g_mlp, g_attn, w_o, w_gate, w_up, w_down, w_q, w_k, w_v)
            o, _, _ = global_attention(p, slots, rows, d, n_chip)(cache_len, q, k, v, kc, vc)
            if p + 1 < pairs:
                x, q, k, v = layer_kernel(l + 1, l + 2, rows, d, ff)(
                    o, x, g_mlp, g_attn, w_o, w_gate, w_up, w_down, w_q, w_k, w_v)
            else:
                x, = layer_kernel(l + 1, None, rows, d, ff)(o, x, g_mlp, w_o, w_gate, w_up, w_down)
        return x

    return jax.shard_map(step, mesh=mesh, in_specs=in_specs, out_specs=row_spec, check_vma=False)
```

```python
import functools
import jax
import jax.numpy as jnp
from jax import lax
from jax.experimental import pallas as pl
from jax.experimental.pallas import tpu as pltpu
from jax.sharding import PartitionSpec as P

EPS = 1e-6
CH = 512
NS = 3
KT = 1024
HU = 5
HD = 128
LOG2E = 1.4426950408889634
SCALE2 = LOG2E * HD ** -0.5
NEG = -jnp.inf
BF = jnp.bfloat16
F32 = jnp.float32
VLIM = 60 * 2 ** 20

VM = pl.BlockSpec(memory_space=pltpu.VMEM)
HB = pl.BlockSpec(memory_space=pl.ANY)
SM = pl.BlockSpec(memory_space=pltpu.SMEM)


def norm_rows(xf, gain):
    inv = lax.rsqrt(jnp.mean(xf * xf, axis=-1, keepdims=True) + EPS)
    return (xf * inv * gain).astype(BF)


def col(c, w):
    return pl.ds(pl.multiple_of(c * w, w), w)


def layer_kernel(layer, nxt, rows, d, ff, local=None, n_proj=3):
    has_tail = layer is not None
    early = local is not None
    heads = d // HD
    na = d // CH if has_tail else 0
    nb = ff // CH if has_tail else 0
    nc = d // CH if nxt is not None else 0
    total = na + nb + nc

    def body(*refs):
        refs = list(refs)

        def take(n):
            out = refs[:n]
            del refs[:n]
            return out
        if local is not None:
            dev_ref, qi_ref, ki_ref, vi_ref, kh_ref, vh_ref, kl_ref, vl_ref = take(8)
        elif has_tail:
            o_ref, = take(1)
        x_ref, = take(1)
        if has_tail:
            gm_ref, = take(1)
        if nc:
            ga_ref, = take(1)
        if has_tail:
            wo, wg, wu, wd = take(4)
        if nc:
            qkv_w = take(n_proj)
        if has_tail:
            xo_ref, = take(1)
        if nc:
            qkv_refs = take(n_proj)
        ba, bb, bc, bd, h_s, acc, sa, sb, sc, sd = take(10)
        if local is not None:
            o_ref, kl_s, vl_s, sl = take(4)

        def cp(w, l, c, buf, sem, slot, by_rows=False):
            src = w.at[l, pl.ds(pl.multiple_of(c * CH, CH), CH), :] if by_rows else w.at[l, :, col(c, CH)]
            return pltpu.make_async_copy(src, buf.at[slot], sem.at[slot])

        def start(t):
            slot = lax.rem(t, NS)
            if has_tail:
                @pl.when(t < na)
                def _():
                    cp(wo, layer, t, bd, sd, slot, True).start()

                @pl.when((t >= na + (NS if early else 0)) & (t < na + nb))
                def _():
                    cp(wg, layer, t - na, ba, sa, slot).start()
                    cp(wu, layer, t - na, bb, sb, slot).start()

                @pl.when((t >= na) & (t < na + nb))
                def _():
                    cp(wd, layer, t - na, bd, sd, slot, True).start()
            if nc:
                @pl.when((t >= na + nb) & (t < total))
                def _():
                    for w, buf, sem in zip(qkv_w, (ba, bb, bc), (sa, sb, sc)):
                        cp(w, nxt, t - na - nb, buf, sem, slot).start()

        def ahead(t):
            if early:
                @pl.when(t >= 1)
                def _():
                    start(t + NS - 1)
            else:
                start(t + NS - 1)

        if local is not None:
            fetch = [pltpu.make_async_copy(src.at[local], dst, sl.at[i])
                     for i, (src, dst) in enumerate(((kl_ref, kl_s), (vl_ref, vl_s)))]
            for f in fetch:
                f.start()
        for t in range(NS if early else NS - 1):
            start(jnp.int32(t))
        if has_tail:
            for c in range(NS if early else 0):
                cp(wg, layer, c, ba, sa, (na + c) % NS).start()
                cp(wu, layer, c, bb, sb, (na + c) % NS).start()
            acc[...] = x_ref[...].astype(F32)
            if local is not None:
                for f in fetch:
                    f.wait()
                first = dev_ref[0] == 0
                key_id = lax.broadcasted_iota(jnp.int32, (rows, rows), 0)
                row_id = lax.broadcasted_iota(jnp.int32, (rows, rows), 1)

                def some_heads(g, _):
                    for j in range(HU):
                        h = g * HU + j
                        c = col(h, HD)
                        q = qi_ref[:, c]
                        kh = jnp.where(first, kl_s[h], kh_ref[:, c])
                        vh = jnp.where(first, vl_s[h], vh_ref[:, c])
                        dims = (((1,), (1,)), ((), ()))
                        sh = lax.dot_general(kh, q, dims, preferred_element_type=F32)
                        so = lax.dot_general(ki_ref[:, c], q, dims, preferred_element_type=F32)
                        sh = jnp.where(key_id > row_id, sh, NEG)
                        so = jnp.where(key_id <= row_id, so, NEG)
                        m = jnp.maximum(jnp.max(sh, axis=0, keepdims=True), jnp.max(so, axis=0, keepdims=True)) * SCALE2
                        ph = jnp.exp2(sh * SCALE2 - m)
                        po = jnp.exp2(so * SCALE2 - m)
                        den = jnp.sum(ph, axis=0, keepdims=True) + jnp.sum(po, axis=0, keepdims=True)
                        dims = (((0,), (0,)), ((), ()))
                        num = (lax.dot_general(vh, ph.astype(BF), dims, preferred_element_type=F32)
                               + lax.dot_general(vi_ref[:, c], po.astype(BF), dims, preferred_element_type=F32))
                        o_ref[:, c] = (num / den).T.astype(BF)
                    return 0
                lax.fori_loop(0, heads // HU, some_heads, 0)

            def pa(t, _):
                ahead(t)
                slot = lax.rem(t, NS)
                cp(wo, layer, 0, bd, sd, slot, True).wait()
                acc[...] += jnp.dot(o_ref[:, col(t, CH)], bd[slot], preferred_element_type=F32)
                return 0
            lax.fori_loop(0, na, pa, 0)
            xm = acc[...].astype(BF).astype(F32)
            h_s[...] = norm_rows(xm, gm_ref[layer:layer + 1, :].astype(F32))
            acc[...] = xm

            def pb(t, _):
                ahead(t)
                slot = lax.rem(t, NS)
                cp(wg, layer, 0, ba, sa, slot).wait()
                gate = jnp.dot(h_s[...], ba[slot], preferred_element_type=F32)
                cp(wu, layer, 0, bb, sb, slot).wait()
                up = jnp.dot(h_s[...], bb[slot], preferred_element_type=F32)
                act = (jax.nn.gelu(gate, approximate=True) * up).astype(BF)
                cp(wd, layer, 0, bd, sd, slot, True).wait()
                acc[...] += jnp.dot(act, bd[slot], preferred_element_type=F32)
                return 0
            lax.fori_loop(na, na + nb, pb, 0)
            xb = acc[...].astype(BF)
            xo_ref[...] = xb
        else:
            xb = x_ref[...]
        if nc:
            h_s[...] = norm_rows(xb.astype(F32), ga_ref[nxt:nxt + 1, :].astype(F32))

            def pc(t, _):
                ahead(t)
                slot = lax.rem(t, NS)
                for w, buf, sem, r in zip(qkv_w, (ba, bb, bc), (sa, sb, sc), qkv_refs):
                    cp(w, nxt, 0, buf, sem, slot).wait()
                    r[:, col(t - na - nb, CH)] = jnp.dot(h_s[...], buf[slot], preferred_element_type=F32).astype(BF)
                return 0
            lax.fori_loop(na + nb, total, pc, 0)

    specs = []
    if local is not None:
        specs += [SM] + [VM] * 5 + [HB] * 2
    elif has_tail:
        specs += [VM]
    specs += [VM] * (1 + (1 if has_tail else 0) + (1 if nc else 0))
    specs += [HB] * ((4 if has_tail else 0) + (n_proj if nc else 0))
    n_out = (1 if has_tail else 0) + (n_proj if nc else 0)
    flops = 2 * rows * d * ((d + 3 * ff if has_tail else 0) + (n_proj * d if nc else 0))
    dma = pltpu.SemaphoreType.DMA
    scratch = [
        pltpu.VMEM((NS, d, CH), BF), pltpu.VMEM((NS, d, CH), BF),
        pltpu.VMEM((NS, d, CH) if nc else (NS, 16, CH), BF), pltpu.VMEM((NS, CH, d), BF),
        pltpu.VMEM((rows, d), BF), pltpu.VMEM((rows, d), F32), dma((NS,)), dma((NS,)), dma((NS,)), dma((NS,))]
    if local is not None:
        scratch += [pltpu.VMEM((rows, d), BF), pltpu.VMEM((heads, rows, HD), BF), pltpu.VMEM((heads, rows, HD), BF), dma((2,))]
    return pl.pallas_call(
        body, out_shape=[jax.ShapeDtypeStruct((rows, d), BF)] * n_out, in_specs=specs, out_specs=[VM] * n_out,
        scratch_shapes=scratch,
        compiler_params=pltpu.CompilerParams(vmem_limit_bytes=VLIM),
        cost_estimate=pl.CostEstimate(flops=flops, bytes_accessed=flops // rows, transcendentals=0),
        name=f"layer_{layer}_{nxt}_{n_proj}")


def global_attention(pair, slot_rows, rows, d, n_chip):
    n_dev = 2 * n_chip
    nq = n_dev * rows
    qh = nq // 2
    heads = d // HD
    hh = heads // 2
    half = hh * HD
    cache = 2 * slot_rows
    keys = cache + 2 * rows
    st = HD + 8
    n_tile = cache // KT
    low = -3e38

    def body(len_ref, q_ref, kn_ref, vn_ref, kc, vc, o_ref, kx, vx,
             qb, knp, vnp, ks, vs, cap, m_s, l_s, acc, s_a, s_b, stage, part,
             q_snd, q_rcv, x_snd, x_rcv, n_snd, n_rcv, p_snd, p_rcv, sk, sv):
        dev = lax.axis_index('ctx')
        core = lax.rem(dev, 2)
        g_me = lax.div(dev, 2)
        mate = dev + 1 - 2 * core

        def remote(src, dst, snd, rcv, to):
            return pltpu.make_async_remote_copy(
                src_ref=src, dst_ref=dst, send_sem=snd, recv_sem=rcv,
                device_id={'ctx': to}, device_id_type=pl.DeviceIdType.MESH)

        def head_cols(b, i):
            return pl.ds(pl.multiple_of((b * hh + i) * HD, HD), HD)

        def dev_rows(t):
            return pl.ds(pl.multiple_of(t * rows, rows), rows)

        def q_copy(i, k):
            to = lax.rem(dev + k, n_dev)
            return remote(q_ref.at[:, head_cols(lax.rem(to, 2), i)], qb.at[i, dev_rows(dev), :],
                          q_snd.at[i, k - 1], q_rcv.at[i, dev], to)

        def q_wait(i, k):
            src = lax.rem(dev + k, n_dev)
            remote(q_ref.at[:, head_cols(0, i)], qb.at[i, dev_rows(src), :],
                   q_snd.at[i, k - 1], q_rcv.at[i, src], src).wait_recv()

        def x_copy(i, w):
            src, dst = ((kc, kx), (vc, vx))[w]
            return remote(src.at[pair, (1 - core) * hh + i], dst.at[i], x_snd.at[w, i], x_rcv.at[w, i], mate)

        def n_copy(w):
            src, dst = ((kn_ref, knp), (vn_ref, vnp))[w]
            return remote(src.at[:, pl.ds(pl.multiple_of((1 - core) * half, half), half)], dst,
                          n_snd.at[w], n_rcv.at[w], mate)

        def p_copy(i, to):
            return remote(stage.at[i, to], part.at[core * hh + i, g_me],
                          p_snd.at[i, to], p_rcv.at[core * hh + i, g_me], to)

        def own(i, slot, w):
            src, dst, sem = ((kc, ks, sk), (vc, vs, sv))[w]
            return pltpu.make_async_copy(src.at[pair, core * hh + i], dst.at[slot, 0:slot_rows, :], sem.at[slot, 0])

        def mated(i, slot, w):
            src, dst, sem = ((kx, ks, sk), (vx, vs, sv))[w]
            return pltpu.make_async_copy(src.at[i], dst.at[slot, slot_rows:cache, :], sem.at[slot, 1])

        bar = pltpu.get_barrier_semaphore()
        for k in range(1, n_dev):
            pl.semaphore_signal(bar, inc=1, device_id={'ctx': lax.rem(dev + k, n_dev)}, device_id_type=pl.DeviceIdType.MESH)
        pl.semaphore_wait(bar, n_dev - 1)

        for w in range(2):
            own(0, 0, w).start()
            x_copy(0, w).start()
            n_copy(w).start()

        def send_q(i, _):
            for k in range(1, n_dev):
                q_copy(i, k).start()
            return 0
        lax.fori_loop(0, hh, send_q, 0)

        def send_x(i, _):
            for w in range(2):
                x_copy(i, w).start()
            return 0
        lax.fori_loop(1, hh, send_x, 0)
        for w in range(2):
            x_copy(0, w).wait_recv()
            mated(0, 0, w).start()
            n_copy(w).wait_recv()

        n = len_ref[0]
        for t, owner in enumerate((dev, mate)):
            left = n - owner * slot_rows
            cap[t * slot_rows:(t + 1) * slot_rows, :] = jnp.where(
                lax.broadcasted_iota(jnp.int32, (slot_rows, HD), 0) < left, -NEG, NEG)

        def one_head(i, _):
            slot = lax.rem(i, 2)

            @pl.when(i + 1 < hh)
            def _():
                for w in range(2):
                    own(i + 1, 1 - slot, w).start()
                    x_copy(i + 1, w).wait_recv()
                    mated(i + 1, 1 - slot, w).start()
            mine = head_cols(core, i)
            there = head_cols(0, i)
            ks[slot, cache:cache + rows, :] = kn_ref[:, mine]
            ks[slot, cache + rows:keys, :] = knp[:, there]
            vs[slot, cache:cache + rows, :] = vn_ref[:, mine]
            vs[slot, cache + rows:keys, :] = vnp[:, there]
            qb[i, dev_rows(dev), :] = q_ref[:, mine]
            for k in range(1, n_dev):
                q_wait(i, k)
            for w in range(2):
                own(i, slot, w).wait()
                mated(i, slot, w).wait()

            def one_half(hf, _):
                q = qb[i, pl.ds(pl.multiple_of(hf * qh, qh), qh), :]
                m_s[...] = jnp.full(m_s.shape, low, F32)
                l_s[...] = jnp.zeros(l_s.shape, F32)
                acc[...] = jnp.zeros(acc.shape, F32)

                def scores(start, size):
                    k = ks[slot, start:start + size, :]
                    return lax.dot_general(k, q, (((1,), (1,)), ((), ())), preferred_element_type=F32)

                def absorb(s, start, size):
                    v = vs[slot, start:start + size, :]
                    m0 = m_s[...]
                    m1 = jnp.maximum(m0, jnp.max(s, axis=0, keepdims=True))
                    a = jnp.exp2((m0 - m1) * SCALE2)
                    p = jnp.exp2(s * SCALE2 - m1 * SCALE2)
                    l_s[...] = l_s[...] * a + jnp.sum(p, axis=0, keepdims=True)
                    m_s[...] = m1
                    acc[...] = acc[...] * a + lax.dot_general(v, p.astype(BF), (((0,), (0,)), ((), ())), preferred_element_type=F32)

                def valid(s, t):
                    lim = cap[t * KT:(t + 1) * KT, :]
                    return jnp.minimum(s, jnp.concatenate([lim] * (qh // HD), axis=1))

                bufs = (s_a, s_b)
                s_b[0:2 * rows, :] = scores(cache, 2 * rows)
                s_a[...] = scores(0, KT)
                s = s_b[0:2 * rows, :]
                r = lax.broadcasted_iota(jnp.int32, s.shape, 0)
                qi = lax.broadcasted_iota(jnp.int32, s.shape, 1) + hf * qh
                pos = jnp.where(r < rows, r + dev * rows, r - rows + mate * rows)
                absorb(jnp.where(pos <= qi, s, NEG), cache, 2 * rows)
                for t in range(n_tile):
                    if t + 1 < n_tile:
                        bufs[(t + 1) % 2][...] = scores((t + 1) * KT, KT)
                    absorb(valid(bufs[t % 2][...], t), t * KT, KT)
                for t in range(n_chip):
                    c = slice(t * rows, (t + 1) * rows)
                    to = hf * n_chip + t
                    stage[i, to, 0:HD, :] = acc[:, c]
                    stage[i, to, HD:HD + 1, :] = m_s[:, c]
                    stage[i, to, HD + 1:HD + 2, :] = l_s[:, c]
                for t in range(n_chip):
                    to = hf * n_chip + t

                    @pl.when(to != dev)
                    def _():
                        p_copy(i, to).start()

                    @pl.when(to == dev)
                    def _():
                        part[core * hh + i, g_me] = stage[i, to]
                return 0
            lax.fori_loop(0, 2, one_half, 0)
            return 0
        lax.fori_loop(0, hh, one_head, 0)

        def finish(i, _):
            for b in range(2):
                h = b * hh + i
                for g in range(n_chip):
                    src = 2 * g + b

                    @pl.when(src != dev)
                    def _():
                        remote(stage.at[i, 0], part.at[h, g], p_snd.at[i, 0], p_rcv.at[h, g], mate).wait_recv()
                m = [part[h, g, HD:HD + 1, :] for g in range(n_chip)]
                top = functools.reduce(jnp.maximum, m)
                num = 0.0
                den = 0.0
                for g in range(n_chip):
                    a = jnp.exp2((m[g] - top) * SCALE2)
                    num = num + part[h, g, 0:HD, :] * a
                    den = den + part[h, g, HD + 1:HD + 2, :] * a
                o_ref[:, head_cols(b, i)] = (num / den).T.astype(BF)
            return 0
        lax.fori_loop(0, hh, finish, 0)

        def drain(i, _):
            for k in range(1, n_dev):
                q_copy(i, k).wait_send()
                p_copy(i, lax.rem(dev + k, n_dev)).wait_send()
            for w in range(2):
                x_copy(i, w).wait_send()
            return 0
        lax.fori_loop(0, hh, drain, 0)
        for w in range(2):
            n_copy(w).wait_send()

    flops = 4 * nq * keys * half
    dma = pltpu.SemaphoreType.DMA
    xs = jax.ShapeDtypeStruct((hh, slot_rows, HD), BF)
    return pl.pallas_call(
        body, out_shape=[jax.ShapeDtypeStruct((rows, d), BF), xs, xs],
        in_specs=[SM, VM, VM, VM, HB, HB], out_specs=[VM, HB, HB],
        scratch_shapes=[
            pltpu.VMEM((hh, nq, HD), BF), pltpu.VMEM((rows, half), BF), pltpu.VMEM((rows, half), BF),
            pltpu.VMEM((2, keys, HD), BF), pltpu.VMEM((2, keys, HD), BF),
            pltpu.VMEM((cache, HD), F32), pltpu.VMEM((1, qh), F32), pltpu.VMEM((1, qh), F32), pltpu.VMEM((HD, qh), F32),
            pltpu.VMEM((KT, qh), F32), pltpu.VMEM((KT, qh), F32),
            pltpu.VMEM((hh, n_dev, st, rows), F32), pltpu.VMEM((heads, n_chip, st, rows), F32),
            dma((hh, n_dev - 1)), dma((hh, n_dev)), dma((2, hh)), dma((2, hh)), dma((2,)), dma((2,)),
            dma((hh, n_dev)), dma((heads, n_chip)), dma((2, 2)), dma((2, 2))],
        compiler_params=pltpu.CompilerParams(vmem_limit_bytes=VLIM, collective_id=pair, has_side_effects=True),
        cost_estimate=pl.CostEstimate(flops=flops, bytes_accessed=4 * keys * half, transcendentals=0),
        name=f"global_{pair}")


def solution(mesh):
    n_dev = mesh.shape['ctx']
    n_chip = n_dev // 2
    shift = [(i, i + 1) for i in range(n_dev - 1)]
    row_spec = P(('dp', 'ctx'), None)
    cache_spec = P(None, ('dp', 'ctx'), None, None)
    local_spec = P(None, 'dp', None, None)
    in_specs = (row_spec, P('dp'), cache_spec, cache_spec, local_spec, local_spec) + (P(),) * 9

    def step(x, cache_len, k_cache, v_cache, k_local, v_local, g_attn, g_mlp, w_q, w_k, w_v, w_o, w_gate, w_up, w_down):
        dev_a = lax.axis_index('ctx').astype(jnp.int32).reshape(1)
        rows, d = x.shape
        ff = w_gate.shape[2]
        pairs, slots, _, _ = k_cache.shape
        kc = jnp.transpose(k_cache, (0, 2, 1, 3))
        vc = jnp.transpose(v_cache, (0, 2, 1, 3))
        kl = jnp.transpose(k_local, (0, 2, 1, 3))
        vl = jnp.transpose(v_local, (0, 2, 1, 3))
        for p in range(pairs):
            l = 2 * p
            xh = lax.ppermute(x, 'ctx', shift)
            q, k, v = layer_kernel(None, l, rows, d, ff)(x, g_attn, w_q, w_k, w_v)
            kh, vh = layer_kernel(None, l, rows, d, ff, n_proj=2)(xh, g_attn, w_k, w_v)
            x, q, k, v = layer_kernel(l, l + 1, rows, d, ff, local=p)(
                dev_a, q, k, v, kh, vh, kl, vl, x, g_mlp, g_attn, w_o, w_gate, w_up, w_down, w_q, w_k, w_v)
            o, _, _ = global_attention(p, slots, rows, d, n_chip)(cache_len, q, k, v, kc, vc)
            x, = layer_kernel(l + 1, None, rows, d, ff)(o, x, g_mlp, w_o, w_gate, w_up, w_down)
        return x

    return jax.shard_map(step, mesh=mesh, in_specs=in_specs, out_specs=row_spec, check_vma=False)
```
